256 devices in a mesh: inst: 4 (over x_hi, core), gx: 8 (over y, x_lo), gy: 8 (over z).
Axes of the slice: x: 4 (x_hi: 2, x_lo: 2; x = x_hi * 2 + x_lo), y: 4, z: 8, core: 2. Of those that a mesh axis runs over, the one named last changes fastest.
Arguments:
- state: float32 [8, 5, 64, 64, 128], P('inst', None, 'gx', 'gy'), may hold values from -6 to 6
- source: float32 [8, 5, 64, 64, 128], P('inst', None, 'gx', 'gy'), may hold values from -60 to 60
- jacobian: float32 [8, 5, 5, 64, 64, 128], P('inst', None, None, 'gx', 'gy'), may hold values from -1.5 to 16, as said below
- couplings: float32 [6, 5, 5], replicated, may hold values from -0.625 to 0.625
- omega: float32 [1], replicated, may hold values from 0.2 to 0.6
Outputs:
- state_next: float32 [8, 5, 64, 64, 128], P('inst', None, 'gx', 'gy')
- last_residual: float32 [8, 5, 64, 64, 128], P('inst', None, 'gx', 'gy')
The draws below stay inside these ranges and needn't reach their ends.
Inputs may be any that keep to these rules, and one draw needn't show every extreme that they name: In every block jacobian[n, :, :, cell] each diagonal entry lies in 8 to 16 and exceeds the sum of magnitudes of the other entries of its row by 2 or more.
All inputs are finite; a program needn't handle non-finite values.
Results may differ from the reference program's by a relative error of at most 0.0003.
Values sent between devices are 32-bit elements; how exact they have to be, the bound alone decides.
A program may use at most 64 MiB of HBM per device.

```python
import math
import jax
import jax.numpy as jnp
from jax import lax

NVAR = 5
NT = 8
ITERS = 3
NX = 64
NY = 64
NZ = 128


def draw_jacobian(key, part):
    first_key, second_key = jax.random.split(jax.random.fold_in(key, 17))
    shape = (NT, NVAR, NVAR, NX, NY, NZ)
    diagonal = jax.random.uniform(first_key, (NT, NVAR, NX, NY, NZ), jnp.float32, 8.0, 16.0)
    others = jnp.clip(0.6 * jax.random.normal(second_key, shape, jnp.float32), -1.5, 1.5)
    identity = jnp.eye(NVAR, dtype=jnp.float32)[None, :, :, None, None, None]
    return others * (1.0 - identity) + identity * diagonal[:, :, None]


def shard_levels(stream_key, shape, shards, least, largest):
    level, own = 1.0, jax.random.fold_in(stream_key, 6)
    for axis_at, blocks in shards:
        heights = jnp.exp(jax.random.uniform(jax.random.fold_in(own, axis_at), (blocks,), jnp.float32, least / len(shards), largest / len(shards)))
        level = level * jnp.repeat(heights, shape[axis_at] // blocks).reshape([-1 if axis == axis_at else 1 for axis in range(len(shape))])
    return level


def bell_draw(key, shape, scale, most, cuts=(), held_as=jnp.bfloat16):
    drawn = scale * jax.random.normal(key, shape, jnp.float32)
    if cuts:
        drawn = drawn * shard_levels(key, shape, cuts, -0.22, 0.18)
    return jnp.clip(drawn, -most, most).astype(held_as)


def setup_inputs(seed: int = 0) -> dict:
    streams_of = jax.random.split(jax.random.key(seed), 6)
    return {
        "state": bell_draw(streams_of[0], (NT, NVAR, NX, NY, NZ), 1.0, 6.0, ((0, 4), (2, 8), (3, 8)), jnp.float32),
        "source": bell_draw(streams_of[1], (NT, NVAR, NX, NY, NZ), 10.0, 60.0, ((0, 4), (2, 8), (3, 8)), jnp.float32),
        "jacobian": draw_jacobian(jax.random.fold_in(streams_of[5], 71), 0),
        "couplings": bell_draw(streams_of[3], (6, NVAR, NVAR), 100 ** -0.5, 0.625, (), jnp.float32),
        "omega": jnp.clip(jnp.exp(jax.random.uniform(streams_of[4], (1,), jnp.float32, math.log(0.2), math.log(0.6))), 0.2, 0.6),
    }


def spectral_table(row_index, column_index, total):
    offset = (row_index[:, None] - column_index[None, :]).astype(jnp.int32)
    parity = 1.0 - 2.0 * jnp.mod(offset, 2).astype(jnp.float32)
    angle = jnp.pi * offset.astype(jnp.float32) / total
    onsite = offset == 0
    sine = jnp.where(onsite, jnp.ones_like(angle), jnp.sin(angle))
    return jnp.where(onsite, jnp.zeros_like(angle), 0.5 * parity * jnp.cos(angle) / sine)


def pad_field(field):
    wrapped = jnp.concatenate([field[:, :, -1:], field, field[:, :, :1]], axis=2)
    return jnp.pad(wrapped, ((0, 0), (1, 1), (0, 0), (1, 1)))


def neighbours(padded, couplings):
    shifted = [padded[:, :-2, 1:-1, 1:-1], padded[:, 2:, 1:-1, 1:-1],
               padded[:, 1:-1, :-2, 1:-1], padded[:, 1:-1, 2:, 1:-1],
               padded[:, 1:-1, 1:-1, :-2], padded[:, 1:-1, 1:-1, 2:]]
    result = jnp.zeros(shifted[0].shape, jnp.float32)
    for direction in range(6):
        result = result + jnp.einsum("vw,wxyz->vxyz", couplings[direction], shifted[direction],
                                     precision=lax.Precision.HIGHEST)
    return result


def solve_blocks(blocks, right):
    size = blocks.shape[0]
    matrix = [[blocks[row, column] for column in range(size)] for row in range(size)]
    vector = [right[row] for row in range(size)]
    for pivot in range(size):
        for target in range(pivot + 1, size):
            factor = matrix[target][pivot] / matrix[pivot][pivot]
            for column in range(pivot + 1, size):
                matrix[target][column] = matrix[target][column] - factor * matrix[pivot][column]
            vector[target] = vector[target] - factor * vector[pivot]
    result = [None] * size
    for pivot in reversed(range(size)):
        total = vector[pivot]
        for column in range(pivot + 1, size):
            total = total - matrix[pivot][column] * result[column]
        result[pivot] = total / matrix[pivot][pivot]
    return jnp.stack(result, axis=0)


def reference(state, source, jacobian, couplings, omega):
    total = state.shape[0]
    positions = jnp.arange(total, dtype=jnp.int32)
    table = spectral_table(positions, positions, total)
    current = state
    residual = state
    for repeat in range(ITERS):
        spectral = omega[0] * jnp.einsum("nm,mvxyz->nvxyz", table, current,
                                         precision=lax.Precision.HIGHEST)

        def one_instance(pieces):
            field, blocks, right_side, spec_part = pieces
            beside = neighbours(pad_field(field), couplings)
            diagonal_part = jnp.einsum("vwxyz,wxyz->vxyz", blocks, field,
                                       precision=lax.Precision.HIGHEST)
            resid = right_side - diagonal_part - beside - spec_part
            return field + solve_blocks(blocks, resid), resid

        current, residual = lax.map(one_instance, (current, jacobian, source, spectral))
    return current, residual
```

```python
import functools
import math

import jax
import jax.numpy as jnp
from jax import lax
from jax.experimental import pallas as pl
from jax.experimental.pallas import tpu as pltpu
from jax.sharding import PartitionSpec as P

ITERS = 3
NV = 5
MESH = pl.DeviceIdType.MESH


def table_value(offset, total):
    angle = math.pi * offset / total
    return 0.5 * (-1.0) ** offset * math.cos(angle) / math.sin(angle)


def kernel(
    state_ref, source_ref, jac_ref, coup_ref, omega_ref,
    out_ref, res_ref,
    cur, src, jac, lu, near, far, fwd, ysend, yrecv, resid, cs,
    load_sem, src_sem, jac_sem, near_sem, far_sem, fwd_sem, y_sem, gx_sem, send_sem, out_sem,
):
    inst, gx, gy = lax.axis_index("inst"), lax.axis_index("gx"), lax.axis_index("gy")
    ngx, ngy, ranks = lax.axis_size("gx"), lax.axis_size("gy"), lax.axis_size("inst")
    nloc, nx = state_ref.shape[0], state_ref.shape[2]
    total = ranks * nloc
    parity = lax.rem(inst, 2)
    other_core = (inst + 1 - 2 * parity, gx, gy)
    other_chip = (lax.rem(inst + 2, ranks), gx, gy)
    gx_low, gx_high = (inst, gx - 1, gy), (inst, gx + 1, gy)
    gy_low = (inst, gx, lax.rem(gy + ngy - 1, ngy))
    gy_high = (inst, gx, lax.rem(gy + 1, ngy))
    has_low, has_high = gx > 0, gx < ngx - 1

    def plane_at(position):
        half = position // 2
        odd = position - 2 * half
        return half + odd * (nx - 1 - 2 * half)

    def load_state(x):
        return pltpu.make_async_copy(state_ref.at[:, :, x], cur.at[0, x + 1], load_sem.at[x])

    def remote(source, target, send, recv, device):
        return pltpu.make_async_remote_copy(
            src_ref=source, dst_ref=target, send_sem=send, recv_sem=recv,
            device_id=device, device_id_type=MESH,
        )

    def near_copy(k, x):
        return remote(cur.at[k, x + 1], near.at[k, x], send_sem.at[0], near_sem.at[k, x], other_core)

    def far_copy(k, x):
        return remote(cur.at[k, x + 1], far.at[k, x], send_sem.at[1], far_sem.at[k, x], other_chip)

    def fwd_copy(k, x):
        return remote(far.at[k, x], fwd.at[k, x], send_sem.at[2], fwd_sem.at[k, x], other_core)

    def y_copy(k, x, d):
        return remote(
            ysend.at[k, x, d], yrecv.at[k, x, d], send_sem.at[3 + d], y_sem.at[k, x, d],
            gy_high if d == 0 else gy_low,
        )

    def gx_copy(k, d):
        if d == 0:
            return remote(cur.at[k, nx], cur.at[k, 0], send_sem.at[5], gx_sem.at[k, 0], gx_high)
        return remote(cur.at[k, 1], cur.at[k, nx + 1], send_sem.at[6], gx_sem.at[k, 1], gx_low)

    def send_plane(k, x):
        far_copy(k, x).start()

        @pl.when((x == 0) & has_low)
        def _():
            gx_copy(k, 1).start()

        @pl.when((x == nx - 1) & has_high)
        def _():
            gx_copy(k, 0).start()

        near_copy(k, x).start()
        y_copy(k, x, 0).start()
        y_copy(k, x, 1).start()

    def start_load(p, c):
        load_state(plane_at(p)).start()
        return c

    lax.fori_loop(0, nx, start_load, 0)
    for n in range(nloc):
        pltpu.make_async_copy(jac_ref.at[n], jac.at[n], jac_sem.at[n]).start()
    pltpu.make_async_copy(source_ref, src, src_sem).start()

    barrier = pltpu.get_barrier_semaphore()
    for device in (other_core, other_chip, gy_low, gy_high):
        pl.semaphore_signal(barrier, inc=1, device_id=device, device_id_type=MESH)

    @pl.when(has_low)
    def _():
        pl.semaphore_signal(barrier, inc=1, device_id=gx_low, device_id_type=MESH)

    @pl.when(has_high)
    def _():
        pl.semaphore_signal(barrier, inc=1, device_id=gx_high, device_id_type=MESH)

    tile = cs.shape[1:]
    for d in range(6):
        for v in range(NV):
            for w in range(NV):
                cs[(d * NV + v) * NV + w] = jnp.full(tile, coup_ref[d, v, w], jnp.float32)
    zeros = jnp.zeros(cur.shape[2:], jnp.float32)

    @pl.when(gx == 0)
    def _():
        for k in range(ITERS):
            cur[k, 0] = zeros

    @pl.when(gx == ngx - 1)
    def _():
        for k in range(ITERS):
            cur[k, nx + 1] = zeros

    pl.semaphore_wait(barrier, 4 + has_low.astype(jnp.int32) + has_high.astype(jnp.int32))

    def put_rows(k, x, n, v, plane):
        ysend[k, x, 0, n, v : v + 1, :] = plane[7:8, :]
        ysend[k, x, 1, n, v : v + 1, :] = plane[0:1, :]

    def first_send(p, c):
        x = plane_at(p)
        load_state(x).wait()
        for n in range(nloc):
            for v in range(NV):
                put_rows(0, x, n, v, cur[0, x + 1, n, v])
        send_plane(0, x)
        return c

    lax.fori_loop(0, nx, first_send, 0)

    for n in range(nloc):
        pltpu.make_async_copy(jac_ref.at[n], jac.at[n], jac_sem.at[n]).wait()

    def factor(x, c):
        for n in range(nloc):
            m = [[jac[n, i, j, x] for j in range(NV)] for i in range(NV)]
            for p in range(NV):
                m[p][p] = 1.0 / m[p][p]
                for t in range(p + 1, NV):
                    m[t][p] = m[t][p] * m[p][p]
                    for j in range(p + 1, NV):
                        m[t][j] = m[t][j] - m[t][p] * m[p][j]
            for i in range(NV):
                for j in range(NV):
                    lu[n, i, j, x] = m[i][j]
        return c

    lax.fori_loop(0, nx, factor, 0)
    pltpu.make_async_copy(source_ref, src, src_sem).wait()

    omega = omega_ref[0]

    def weight(even, odd):
        return omega * jnp.where(parity == 0, jnp.float32(even), jnp.float32(odd))

    value = functools.partial(table_value, total=total)
    own_w = [[None if j == m else omega * jnp.float32(value(j - m)) for m in range(nloc)] for j in range(nloc)]
    near_w = [[weight(value(j - m - 2), value(j - m + 2)) for m in range(nloc)] for j in range(nloc)]
    far_w = [[omega * jnp.float32(value(j - m + 4)) for m in range(nloc)] for j in range(nloc)]
    fwd_w = [[weight(value(j - m + 2), value(j - m - 2)) for m in range(nloc)] for j in range(nloc)]

    def forward(step):
        k = step // nx
        x = plane_at(step - k * nx)
        far_copy(k, x).wait_recv()
        fwd_copy(k, x).start()

    def output_copies(x):
        return (
            pltpu.make_async_copy(cur.at[ITERS, x + 1], out_ref.at[:, :, x], out_sem.at[0, x]),
            pltpu.make_async_copy(resid.at[x], res_ref.at[:, :, x], out_sem.at[1, x]),
        )

    def compute(step):
        k = step // nx
        x = plane_at(step - k * nx)
        near_copy(k, x).wait_recv()
        y_copy(k, x, 0).wait_recv()
        y_copy(k, x, 1).wait_recv()

        @pl.when((x == 0) & has_low)
        def _():
            gx_copy(k, 0).wait_recv()

        @pl.when((x == nx - 1) & has_high)
        def _():
            gx_copy(k, 1).wait_recv()

        fwd_copy(k, x).wait_recv()

        lane = lax.broadcasted_iota(jnp.int32, tile, 1)
        row = lax.broadcasted_iota(jnp.int32, tile, 0)
        ny, nz = tile
        pairs = [(n, v) for n in range(nloc) for v in range(NV)]

        def shifted(d, n, w):
            if d < 2:
                return cur[k, x + 2 * d, n, w]
            plane = cur[k, x + 1, n, w]
            if d == 2:
                return jnp.where(row == 0, yrecv[k, x, 0, n, w : w + 1, :], pltpu.roll(plane, 1, 0))
            if d == 3:
                return jnp.where(row == ny - 1, yrecv[k, x, 1, n, w : w + 1, :], pltpu.roll(plane, ny - 1, 0))
            if d == 4:
                return jnp.where(lane == 0, 0.0, pltpu.roll(plane, 1, 1))
            return jnp.where(lane == nz - 1, 0.0, pltpu.roll(plane, nz - 1, 1))

        total_of = {}
        for n, v in pairs:
            total_of[n, v] = src[n, v, x]
        for n in range(nloc):
            mine = [cur[k, x + 1, n, w] for w in range(NV)]
            for v in range(NV):
                for w in range(NV):
                    total_of[n, v] = total_of[n, v] - jac[n, v, w, x] * mine[w]
        for d in range(6):
            field = {(n, w): shifted(d, n, w) for n, w in pairs}
            for v in range(NV):
                for w in range(NV):
                    c = cs[(d * NV + v) * NV + w]
                    for n in range(nloc):
                        total_of[n, v] = total_of[n, v] - c * field[n, w]
        for v in range(NV):
            own = [cur[k, x + 1, m, v] for m in range(nloc)]
            beside = [near[k, x, m, v] for m in range(nloc)]
            across = [far[k, x, m, v] for m in range(nloc)]
            relayed = [fwd[k, x, m, v] for m in range(nloc)]
            for j in range(nloc):
                acc = total_of[j, v]
                for weights, values in ((own_w, own), (near_w, beside), (far_w, across), (fwd_w, relayed)):
                    for m in range(nloc):
                        if weights[j][m] is not None:
                            acc = acc - weights[j][m] * values[m]
                total_of[j, v] = acc
        for n in range(nloc):
            b = [total_of[n, v] for v in range(NV)]
            for v in range(NV):
                resid[x, n, v] = b[v]
            for p in range(NV):
                for t in range(p + 1, NV):
                    b[t] = b[t] - lu[n, t, p, x] * b[p]
            for p in reversed(range(NV)):
                for j in range(p + 1, NV):
                    b[p] = b[p] - lu[n, p, j, x] * b[j]
                b[p] = b[p] * lu[n, p, p, x]
            for v in range(NV):
                plane = cur[k, x + 1, n, v] + b[v]
                cur[k + 1, x + 1, n, v] = plane
                put_rows(k + 1, x, n, v, plane)

        @pl.when(k < ITERS - 1)
        def _():
            send_plane(k + 1, x)

        @pl.when(k == ITERS - 1)
        def _():
            for copy in output_copies(x):
                copy.start()

    forward(0)

    def one_step(step, c):
        @pl.when(step + 1 < ITERS * nx)
        def _():
            forward(step + 1)

        compute(step)
        return c

    lax.fori_loop(0, ITERS * nx, one_step, 0)

    remote(near, near, send_sem.at[0], near_sem.at[0, 0], other_core).wait_send()
    remote(far, far, send_sem.at[1], far_sem.at[0, 0], other_chip).wait_send()
    remote(fwd, fwd, send_sem.at[2], fwd_sem.at[0, 0], other_core).wait_send()
    for d in range(2):
        sent = yrecv.at[:, :, d]
        remote(sent, sent, send_sem.at[3 + d], y_sem.at[0, 0, d], gy_high).wait_send()

    planes = near.at[0, pl.ds(0, ITERS)]

    @pl.when(has_high)
    def _():
        remote(planes, planes, send_sem.at[5], gx_sem.at[0, 0], gx_high).wait_send()

    @pl.when(has_low)
    def _():
        remote(planes, planes, send_sem.at[6], gx_sem.at[0, 1], gx_low).wait_send()

    def finish(x, c):
        for copy in output_copies(x):
            copy.wait()
        return c

    lax.fori_loop(0, nx, finish, 0)


def shards(state, source, jacobian, couplings, omega):
    nloc, nv, nx, ny, nz = state.shape
    whole = pl.BlockSpec(memory_space=pl.ANY)
    scalars = pl.BlockSpec(memory_space=pltpu.SMEM)
    f32 = jnp.float32
    dma = pltpu.SemaphoreType.DMA
    plane = (nloc, nv, ny, nz)
    out = jax.ShapeDtypeStruct(state.shape, f32)
    return pl.pallas_call(
        kernel,
        out_shape=(out, out),
        in_specs=[whole, whole, whole, scalars, scalars],
        out_specs=(whole, whole),
        scratch_shapes=[
            pltpu.VMEM((ITERS + 1, nx + 2) + plane, f32),
            pltpu.VMEM(source.shape, f32),
            pltpu.VMEM(jacobian.shape, f32),
            pltpu.VMEM(jacobian.shape, f32),
            pltpu.VMEM((ITERS, nx) + plane, f32),
            pltpu.VMEM((ITERS, nx) + plane, f32),
            pltpu.VMEM((ITERS, nx) + plane, f32),
            pltpu.VMEM((ITERS + 1, nx, 2, nloc, 8, nz), f32),
            pltpu.VMEM((ITERS, nx, 2, nloc, 8, nz), f32),
            pltpu.VMEM((nx,) + plane, f32),
            pltpu.VMEM((6 * NV * NV, ny, nz), f32),
            dma((nx,)),
            dma,
            dma((nloc,)),
            dma((ITERS, nx)),
            dma((ITERS, nx)),
            dma((ITERS, nx)),
            dma((ITERS, nx, 2)),
            dma((ITERS, 2)),
            dma((7,)),
            dma((2, nx)),
        ],
        compiler_params=pltpu.CompilerParams(collective_id=0, has_side_effects=True),
    )(state, source, jacobian, couplings, omega)


def solution(mesh):
    return jax.shard_map(
        shards,
        mesh=mesh,
        in_specs=(
            P("inst", None, "gx", "gy", None),
            P("inst", None, "gx", "gy", None),
            P("inst", None, None, "gx", "gy", None),
            P(),
            P(),
        ),
        out_specs=(P("inst", None, "gx", "gy", None), P("inst", None, "gx", "gy", None)),
        check_vma=False,
    )
```

```python
import functools
import math

import jax
import jax.numpy as jnp
from jax import lax
from jax.experimental import pallas as pl
from jax.experimental.pallas import tpu as pltpu
from jax.sharding import PartitionSpec as P

ITERS = 3
OUTER_FIRST, OUTER_STEP, RELAY_LAG = 3, 2, 4
NV = 5
MESH = pl.DeviceIdType.MESH


def table_value(offset, total):
    angle = math.pi * offset / total
    return 0.5 * (-1.0) ** offset * math.cos(angle) / math.sin(angle)


def kernel(
    state_ref, source_ref, jac_ref, coup_ref, omega_ref,
    out_ref, res_ref,
    cur, src, jac, lu, near, far, fwd, ysend, yrecv, cs,
    load_sem, src_sem, jac_sem, near_sem, far_sem, fwd_sem, y_sem, gx_sem, send_sem,
):
    inst, gx, gy = lax.axis_index("inst"), lax.axis_index("gx"), lax.axis_index("gy")
    ngx, ngy, ranks = lax.axis_size("gx"), lax.axis_size("gy"), lax.axis_size("inst")
    nloc, nx = state_ref.shape[0], state_ref.shape[2]
    total = ranks * nloc
    parity = lax.rem(inst, 2)
    other_core = (inst + 1 - 2 * parity, gx, gy)
    other_chip = (lax.rem(inst + 2, ranks), gx, gy)
    odd = lax.rem(gx, 2)
    mate = (inst, gx + 1 - 2 * odd, gy)
    outer = odd * (nx - 1)
    inner = nx - 1 - outer
    step_out = 2 * odd - 1
    has_outer = jnp.where(odd == 0, gx > 0, gx < ngx - 1)
    outside = (lax.rem(inst + 2, ranks), gx + step_out, gy)
    gy_low = (inst, gx, lax.rem(gy + ngy - 1, ngy))
    gy_high = (inst, gx, lax.rem(gy + 1, ngy))

    def outer_at(k):
        return jnp.minimum(OUTER_FIRST + OUTER_STEP * k, nx - 1)

    def plane_at(position, at):
        distance = jnp.where(position < at, nx - 1 - position, jnp.where(position > at, nx - position, 0))
        return outer + (1 - 2 * odd) * distance

    def load_state(x):
        return pltpu.make_async_copy(state_ref.at[:, :, x], cur.at[0, x + 1], load_sem.at[x])

    def remote(source, target, send, recv, device):
        return pltpu.make_async_remote_copy(
            src_ref=source, dst_ref=target, send_sem=send, recv_sem=recv,
            device_id=device, device_id_type=MESH,
        )

    def near_copy(k, x):
        return remote(cur.at[k, x + 1], near.at[k, x], send_sem.at[0], near_sem.at[k, x], other_core)

    def far_copy(k, x):
        return remote(cur.at[k, x + 1], far.at[k, x], send_sem.at[1], far_sem.at[k, x], other_chip)

    def fwd_copy(k, x):
        return remote(far.at[k, x], fwd.at[k, x], send_sem.at[2], fwd_sem.at[k, x], other_core)

    def y_copy(k, x, d):
        return remote(
            ysend.at[k, x, d], yrecv.at[k, x, d], send_sem.at[3 + d], y_sem.at[k, x, d],
            gy_high if d == 0 else gy_low,
        )

    def inner_copy(k):
        return remote(cur.at[k, inner + 1], cur.at[k, odd * (nx + 1)], send_sem.at[5], gx_sem.at[k, 0], mate)

    def outer_copy(k):
        return remote(far.at[k, outer], cur.at[k, (1 - odd) * (nx + 1)], send_sem.at[6], gx_sem.at[k, 1], outside)

    def send_plane(k, x):
        @pl.when(x == inner)
        def _():
            inner_copy(k).start()

        far_copy(k, x).start()
        near_copy(k, x).start()
        y_copy(k, x, 0).start()
        y_copy(k, x, 1).start()

    def start_load(p, c):
        load_state(plane_at(p, 0)).start()
        return c

    lax.fori_loop(0, nx, start_load, 0)
    for n in range(nloc):
        pltpu.make_async_copy(jac_ref.at[n], jac.at[n], jac_sem.at[n]).start()
    pltpu.make_async_copy(source_ref, src, src_sem).start()

    barrier = pltpu.get_barrier_semaphore()
    for device in (other_core, other_chip, mate, gy_low, gy_high):
        pl.semaphore_signal(barrier, inc=1, device_id=device, device_id_type=MESH)

    @pl.when(has_outer)
    def _():
        pl.semaphore_signal(barrier, inc=1, device_id=outside, device_id_type=MESH)

    tile = cs.shape[1:]
    for d in range(6):
        for v in range(NV):
            for w in range(NV):
                cs[(d * NV + v) * NV + w] = jnp.full(tile, coup_ref[v, d, w], jnp.float32)
    zeros = jnp.zeros(cur.shape[2:], jnp.float32)

    @pl.when(gx == 0)
    def _():
        for k in range(ITERS):
            cur[k, 0] = zeros

    @pl.when(gx == ngx - 1)
    def _():
        for k in range(ITERS):
            cur[k, nx + 1] = zeros

    pl.semaphore_wait(barrier, 5 + has_outer.astype(jnp.int32))

    def put_rows(k, x, n, v, plane):
        ysend[k, x, 0, n, v : v + 1, :] = plane[7:8, :]
        ysend[k, x, 1, n, v : v + 1, :] = plane[0:1, :]

    def first_send(p, c):
        x = plane_at(p, 0)
        load_state(x).wait()
        for n in range(nloc):
            for v in range(NV):
                put_rows(0, x, n, v, cur[0, x + 1, n, v])
        send_plane(0, x)
        return c

    lax.fori_loop(0, nx, first_send, 0)

    for n in range(nloc):
        pltpu.make_async_copy(jac_ref.at[n], jac.at[n], jac_sem.at[n]).wait()

    def factor(x, c):
        for n in range(nloc):
            m = [[jac[n, i, j, x] for j in range(NV)] for i in range(NV)]
            for p in range(NV):
                m[p][p] = 1.0 / m[p][p]
                for t in range(p + 1, NV):
                    m[t][p] = m[t][p] * m[p][p]
                    for j in range(p + 1, NV):
                        m[t][j] = m[t][j] - m[t][p] * m[p][j]
            for i in range(NV):
                for j in range(NV):
                    lu[n, i, j, x] = m[i][j]
        return c

    lax.fori_loop(0, nx, factor, 0)
    pltpu.make_async_copy(source_ref, src, src_sem).wait()

    omega = omega_ref[0]

    def weight(even, odd):
        return omega * jnp.where(parity == 0, jnp.float32(even), jnp.float32(odd))

    value = functools.partial(table_value, total=total)
    own_w = [[None if j == m else omega * jnp.float32(value(j - m)) for m in range(nloc)] for j in range(nloc)]
    near_w = [[weight(value(j - m - 2), value(j - m + 2)) for m in range(nloc)] for j in range(nloc)]
    far_w = [[omega * jnp.float32(value(j - m + 4)) for m in range(nloc)] for j in range(nloc)]
    fwd_w = [[weight(value(j - m + 2), value(j - m - 2)) for m in range(nloc)] for j in range(nloc)]

    def forward(step):
        k = step // nx
        x = plane_at(step - k * nx, outer_at(k))

        @pl.when(x != outer)
        def _():
            far_copy(k, x).wait_recv()
            fwd_copy(k, x).start()

    def forward_outer(k):
        far_copy(k, outer).wait_recv()

        @pl.when(has_outer)
        def _():
            outer_copy(k).start()

        fwd_copy(k, outer).start()

    def compute(step):
        k = step // nx
        x = plane_at(step - k * nx, outer_at(k))
        near_copy(k, x).wait_recv()
        y_copy(k, x, 0).wait_recv()
        y_copy(k, x, 1).wait_recv()

        @pl.when(x == inner)
        def _():
            inner_copy(k).wait_recv()

        @pl.when((x == outer) & has_outer)
        def _():
            outer_copy(k).wait_recv()

        fwd_copy(k, x).wait_recv()

        lane = lax.broadcasted_iota(jnp.int32, tile, 1)
        row = lax.broadcasted_iota(jnp.int32, tile, 0)
        ny, nz = tile
        pairs = [(n, v) for n in range(nloc) for v in range(NV)]

        def shifted(d, n, w):
            if d < 2:
                return cur[k, x + 2 * d, n, w]
            plane = cur[k, x + 1, n, w]
            if d == 2:
                return jnp.where(row == 0, yrecv[k, x, 0, n, w : w + 1, :], pltpu.roll(plane, 1, 0))
            if d == 3:
                return jnp.where(row == ny - 1, yrecv[k, x, 1, n, w : w + 1, :], pltpu.roll(plane, ny - 1, 0))
            if d == 4:
                return jnp.where(lane == 0, 0.0, pltpu.roll(plane, 1, 1))
            return jnp.where(lane == nz - 1, 0.0, pltpu.roll(plane, nz - 1, 1))

        total_of = {}
        for n, v in pairs:
            total_of[n, v] = src[n, v, x]
        for n in range(nloc):
            mine = [cur[k, x + 1, n, w] for w in range(NV)]
            for v in range(NV):
                for w in range(NV):
                    total_of[n, v] = total_of[n, v] - jac[n, v, w, x] * mine[w]
        for d in range(6):
            field = {(n, w): shifted(d, n, w) for n, w in pairs}
            for v in range(NV):
                for w in range(NV):
                    c = cs[(d * NV + v) * NV + w]
                    for n in range(nloc):
                        total_of[n, v] = total_of[n, v] - c * field[n, w]
        for v in range(NV):
            own = [cur[k, x + 1, m, v] for m in range(nloc)]
            beside = [near[k, x, m, v] for m in range(nloc)]
            across = [far[k, x, m, v] for m in range(nloc)]
            relayed = [fwd[k, x, m, v] for m in range(nloc)]
            for j in range(nloc):
                acc = total_of[j, v]
                for weights, values in ((own_w, own), (near_w, beside), (far_w, across), (fwd_w, relayed)):
                    for m in range(nloc):
                        if weights[j][m] is not None:
                            acc = acc - weights[j][m] * values[m]
                total_of[j, v] = acc
        for n in range(nloc):
            b = [total_of[n, v] for v in range(NV)]
            for v in range(NV):
                res_ref[n, v, x] = b[v]
            for p in range(NV):
                for t in range(p + 1, NV):
                    b[t] = b[t] - lu[n, t, p, x] * b[p]
            for p in reversed(range(NV)):
                for j in range(p + 1, NV):
                    b[p] = b[p] - lu[n, p, j, x] * b[j]
                b[p] = b[p] * lu[n, p, p, x]
            for v in range(NV):
                plane = cur[k, x + 1, n, v] + b[v]
                out_ref[n, v, x] = plane
                cur[k + 1, x + 1, n, v] = plane
                put_rows(k + 1, x, n, v, plane)

        @pl.when(k < ITERS - 1)
        def _():
            send_plane(k + 1, x)

    forward_outer(0)
    forward(0)

    def one_step(step, c):
        for k in range(1, ITERS):

            @pl.when(step == (k - 1) * nx + outer_at(k - 1) + RELAY_LAG)
            def _():
                forward_outer(k)

        @pl.when(step + 1 < ITERS * nx)
        def _():
            forward(step + 1)

        compute(step)
        return c

    lax.fori_loop(0, ITERS * nx, one_step, 0)

    remote(near, near, send_sem.at[0], near_sem.at[0, 0], other_core).wait_send()
    remote(far, far, send_sem.at[1], far_sem.at[0, 0], other_chip).wait_send()
    remote(fwd, fwd, send_sem.at[2], fwd_sem.at[0, 0], other_core).wait_send()
    for d in range(2):
        sent = yrecv.at[:, :, d]
        remote(sent, sent, send_sem.at[3 + d], y_sem.at[0, 0, d], gy_high).wait_send()

    planes = near.at[0, pl.ds(0, ITERS)]
    remote(planes, planes, send_sem.at[5], gx_sem.at[0, 0], mate).wait_send()

    @pl.when(has_outer)
    def _():
        remote(planes, planes, send_sem.at[6], gx_sem.at[0, 1], outside).wait_send()


def shards(state, source, jacobian, couplings, omega):
    nloc, nv, nx, ny, nz = state.shape
    whole = pl.BlockSpec(memory_space=pltpu.HBM)
    in_hbm = functools.partial(pltpu.with_memory_space_constraint, memory_space=pltpu.HBM)
    scalars = pl.BlockSpec(memory_space=pltpu.SMEM)
    f32 = jnp.float32
    dma = pltpu.SemaphoreType.DMA
    plane = (nloc, nv, ny, nz)
    out = pltpu.VMEM(state.shape, f32)
    return pl.pallas_call(
        kernel,
        out_shape=(out, out),
        in_specs=[whole, whole, whole, scalars, scalars],
        out_specs=(pl.BlockSpec(memory_space=pltpu.VMEM),) * 2,
        scratch_shapes=[
            pltpu.VMEM((ITERS + 1, nx + 2) + plane, f32),
            pltpu.VMEM(source.shape, f32),
            pltpu.VMEM(jacobian.shape, f32),
            pltpu.VMEM(jacobian.shape, f32),
            pltpu.VMEM((ITERS, nx) + plane, f32),
            pltpu.VMEM((ITERS, nx) + plane, f32),
            pltpu.VMEM((ITERS, nx) + plane, f32),
            pltpu.VMEM((ITERS + 1, nx, 2, nloc, 8, nz), f32),
            pltpu.VMEM((ITERS, nx, 2, nloc, 8, nz), f32),
            pltpu.VMEM((6 * NV * NV, ny, nz), f32),
            dma((nx,)),
            dma,
            dma((nloc,)),
            dma((ITERS, nx)),
            dma((ITERS, nx)),
            dma((ITERS, nx)),
            dma((ITERS, nx, 2)),
            dma((ITERS, 2)),
            dma((7,)),
        ],
        compiler_params=pltpu.CompilerParams(collective_id=0, has_side_effects=True, vmem_limit_bytes=24 * 2**20),
    )(in_hbm(state), in_hbm(source), in_hbm(jacobian), jnp.transpose(couplings, (1, 0, 2)), omega)


def solution(mesh):
    return jax.shard_map(
        shards,
        mesh=mesh,
        in_specs=(
            P("inst", None, "gx", "gy", None),
            P("inst", None, "gx", "gy", None),
            P("inst", None, None, "gx", "gy", None),
            P(),
            P(),
        ),
        out_specs=(P("inst", None, "gx", "gy", None), P("inst", None, "gx", "gy", None)),
        check_vma=False,
    )
```

```python
import functools
import math

import jax
import jax.numpy as jnp
from jax import lax
from jax.experimental import pallas as pl
from jax.experimental.pallas import tpu as pltpu
from jax.sharding import PartitionSpec as P

ITERS = 3
OUTER_FIRST, OUTER_STEP, RELAY_LAG = 3, 2, 4
NV = 5
MESH = pl.DeviceIdType.MESH


def table_value(offset, total):
    angle = math.pi * offset / total
    return 0.5 * (-1.0) ** offset * math.cos(angle) / math.sin(angle)


def kernel(
    state_ref, source_ref, jac_ref, coup_ref, omega_ref,
    out_ref, res_ref,
    cur, src, jac, lu, near, far, fwd, ysend, yrecv, cs, coup,
    load_sem, src_sem, jac_sem, near_sem, far_sem, fwd_sem, y_sem, gx_sem, send_sem, coup_sem, group_sem,
):
    inst, gx, gy = lax.axis_index("inst"), lax.axis_index("gx"), lax.axis_index("gy")
    ngx, ngy, ranks = lax.axis_size("gx"), lax.axis_size("gy"), lax.axis_size("inst")
    nloc, nx = state_ref.shape[0], state_ref.shape[2]
    total = ranks * nloc
    parity = lax.rem(inst, 2)
    other_core = (inst + 1 - 2 * parity, gx, gy)
    other_chip = (lax.rem(inst + 2, ranks), gx, gy)
    odd = lax.rem(gx, 2)
    mate = (inst, gx + 1 - 2 * odd, gy)
    outer = odd * (nx - 1)
    inner = nx - 1 - outer
    step_out = 2 * odd - 1
    has_outer = jnp.where(odd == 0, gx > 0, gx < ngx - 1)
    outside = (lax.rem(inst + 2, ranks), gx + step_out, gy)
    gy_low = (inst, gx, lax.rem(gy + ngy - 1, ngy))
    gy_high = (inst, gx, lax.rem(gy + 1, ngy))

    def outer_at(k):
        return jnp.minimum(OUTER_FIRST + OUTER_STEP * k, nx - 1)

    def plane_at(position, at):
        distance = jnp.where(position < at, nx - 1 - position, jnp.where(position > at, nx - position, 0))
        return outer + (1 - 2 * odd) * distance

    def load_state(x):
        return pltpu.make_async_copy(state_ref.at[:, :, x], cur.at[0, x + 1], load_sem.at[x])

    def remote(source, target, send, recv, device):
        return pltpu.make_async_remote_copy(
            src_ref=source, dst_ref=target, send_sem=send, recv_sem=recv,
            device_id=device, device_id_type=MESH,
        )

    def near_copy(k, x):
        return remote(cur.at[k, x + 1], near.at[k, x], send_sem.at[0], near_sem.at[k, x], other_core)

    def far_copy(k, x):
        return remote(cur.at[k, x + 1], far.at[k, x], send_sem.at[1], far_sem.at[k, x], other_chip)

    def fwd_copy(k, x):
        return remote(far.at[k, x], fwd.at[k, x], send_sem.at[2], fwd_sem.at[k, x], other_core)

    def y_copy(k, x, d):
        return remote(
            ysend.at[k, x, d], yrecv.at[k, x, d], send_sem.at[3 + d], y_sem.at[k, x, d],
            gy_high if d == 0 else gy_low,
        )

    def inner_copy(k):
        return remote(cur.at[k, inner + 1], cur.at[k, odd * (nx + 1)], send_sem.at[5], gx_sem.at[k, 0], mate)

    def outer_copy(k):
        return remote(far.at[k, outer], cur.at[k, (1 - odd) * (nx + 1)], send_sem.at[6], gx_sem.at[k, 1], outside)

    def send_plane(k, x):
        @pl.when(x == inner)
        def _():
            inner_copy(k).start()

        far_copy(k, x).start()
        near_copy(k, x).start()

    def send_rows(k, x):
        y_copy(k, x, 0).start()
        y_copy(k, x, 1).start()

    pltpu.make_async_copy(coup_ref, coup, coup_sem).start()
    def start_load(p, c):
        load_state(plane_at(p, 0)).start()
        return c

    lax.fori_loop(0, nx, start_load, 0)
    for n in range(nloc):
        pltpu.make_async_copy(jac_ref.at[n], jac.at[n], jac_sem.at[n]).start()
    pltpu.make_async_copy(source_ref, src, src_sem).start()

    even_here, odd_here = (inst - parity, gx, gy), (inst - parity + 1, gx, gy)
    even_far = (lax.rem(inst - parity + 2, ranks), gx, gy)

    def odd_core(device):
        return (device[0] - parity + 1, device[1], device[2])

    barrier = pltpu.get_barrier_semaphore()

    def greet(device):
        pl.semaphore_signal(barrier, inc=1, device_id=device, device_id_type=MESH)

    greet(even_far)

    @pl.when(parity == 1)
    def _():
        greet(even_here)

    for device in (mate, gy_low, gy_high):
        greet(odd_core(device))

    @pl.when(has_outer)
    def _():
        greet(odd_core(outside))

    @pl.when(parity == 0)
    def _():
        pl.semaphore_wait(barrier, 3)
        pl.semaphore_signal(group_sem, inc=1, device_id=odd_here, device_id_type=MESH)

    @pl.when(parity == 1)
    def _():
        pl.semaphore_wait(group_sem, 1)

    def meet_neighbours():
        @pl.when(parity == 1)
        def _():
            pl.semaphore_wait(barrier, 6 + 2 * has_outer.astype(jnp.int32))
            pl.semaphore_signal(group_sem, inc=1, device_id=even_here, device_id_type=MESH)

        @pl.when(parity == 0)
        def _():
            pl.semaphore_wait(group_sem, 1)

    def put_rows(k, x, n, v, plane):
        ysend[k, x, 0, n, v : v + 1, :] = plane[7:8, :]
        ysend[k, x, 1, n, v : v + 1, :] = plane[0:1, :]

    def first_send(p, c):
        x = plane_at(p, 0)
        load_state(x).wait()
        far_copy(0, x).start()
        near_copy(0, x).start()
        for n in range(nloc):
            for v in range(NV):
                put_rows(0, x, n, v, cur[0, x + 1, n, v])
        return c

    def first_rows(p, c):
        send_rows(0, plane_at(p, 0))
        return c

    lax.fori_loop(0, nx, first_send, 0)

    tile = cs.shape[1:]
    pltpu.make_async_copy(coup_ref, coup, coup_sem).wait()
    for d in range(6):
        for v in range(NV):
            for w in range(NV):
                cs[(d * NV + v) * NV + w] = jnp.full(tile, coup[v, d, w], jnp.float32)
    zeros = jnp.zeros(cur.shape[2:], jnp.float32)

    @pl.when(gx == 0)
    def _():
        for k in range(ITERS):
            cur[k, 0] = zeros

    @pl.when(gx == ngx - 1)
    def _():
        for k in range(ITERS):
            cur[k, nx + 1] = zeros

    for n in range(nloc):
        pltpu.make_async_copy(jac_ref.at[n], jac.at[n], jac_sem.at[n]).wait()

    def factor(x, c):
        for n in range(nloc):
            m = [[jac[n, i, j, x] for j in range(NV)] for i in range(NV)]
            for p in range(NV):
                m[p][p] = 1.0 / m[p][p]
                for t in range(p + 1, NV):
                    m[t][p] = m[t][p] * m[p][p]
                    for j in range(p + 1, NV):
                        m[t][j] = m[t][j] - m[t][p] * m[p][j]
            for i in range(NV):
                for j in range(NV):
                    lu[n, i, j, x] = m[i][j]
        return c

    lax.fori_loop(0, nx, factor, 0)
    pltpu.make_async_copy(source_ref, src, src_sem).wait()
    meet_neighbours()
    inner_copy(0).start()
    lax.fori_loop(0, nx, first_rows, 0)

    omega = omega_ref[0]

    def weight(even, odd):
        return omega * jnp.where(parity == 0, jnp.float32(even), jnp.float32(odd))

    value = functools.partial(table_value, total=total)
    own_w = [[None if j == m else omega * jnp.float32(value(j - m)) for m in range(nloc)] for j in range(nloc)]
    near_w = [[weight(value(j - m - 2), value(j - m + 2)) for m in range(nloc)] for j in range(nloc)]
    far_w = [[omega * jnp.float32(value(j - m + 4)) for m in range(nloc)] for j in range(nloc)]
    fwd_w = [[weight(value(j - m + 2), value(j - m - 2)) for m in range(nloc)] for j in range(nloc)]

    def forward(step):
        k = step // nx
        x = plane_at(step - k * nx, outer_at(k))

        @pl.when(x != outer)
        def _():
            far_copy(k, x).wait_recv()
            fwd_copy(k, x).start()

    def forward_outer(k):
        far_copy(k, outer).wait_recv()

        @pl.when(has_outer)
        def _():
            outer_copy(k).start()

        fwd_copy(k, outer).start()

    def compute(step):
        k = step // nx
        x = plane_at(step - k * nx, outer_at(k))
        near_copy(k, x).wait_recv()
        y_copy(k, x, 0).wait_recv()
        y_copy(k, x, 1).wait_recv()

        @pl.when(x == inner)
        def _():
            inner_copy(k).wait_recv()

        @pl.when((x == outer) & has_outer)
        def _():
            outer_copy(k).wait_recv()

        fwd_copy(k, x).wait_recv()

        lane = lax.broadcasted_iota(jnp.int32, tile, 1)
        row = lax.broadcasted_iota(jnp.int32, tile, 0)
        ny, nz = tile
        pairs = [(n, v) for n in range(nloc) for v in range(NV)]

        def shifted(d, n, w):
            if d < 2:
                return cur[k, x + 2 * d, n, w]
            plane = cur[k, x + 1, n, w]
            if d == 2:
                return jnp.where(row == 0, yrecv[k, x, 0, n, w : w + 1, :], pltpu.roll(plane, 1, 0))
            if d == 3:
                return jnp.where(row == ny - 1, yrecv[k, x, 1, n, w : w + 1, :], pltpu.roll(plane, ny - 1, 0))
            if d == 4:
                return jnp.where(lane == 0, 0.0, pltpu.roll(plane, 1, 1))
            return jnp.where(lane == nz - 1, 0.0, pltpu.roll(plane, nz - 1, 1))

        total_of = {}
        for n, v in pairs:
            total_of[n, v] = src[n, v, x]
        for n in range(nloc):
            mine = [cur[k, x + 1, n, w] for w in range(NV)]
            for v in range(NV):
                for w in range(NV):
                    total_of[n, v] = total_of[n, v] - jac[n, v, w, x] * mine[w]
        for d in range(6):
            field = {(n, w): shifted(d, n, w) for n, w in pairs}
            for v in range(NV):
                for w in range(NV):
                    c = cs[(d * NV + v) * NV + w]
                    for n in range(nloc):
                        total_of[n, v] = total_of[n, v] - c * field[n, w]
        for v in range(NV):
            own = [cur[k, x + 1, m, v] for m in range(nloc)]
            beside = [near[k, x, m, v] for m in range(nloc)]
            across = [far[k, x, m, v] for m in range(nloc)]
            relayed = [fwd[k, x, m, v] for m in range(nloc)]
            for j in range(nloc):
                acc = total_of[j, v]
                for weights, values in ((own_w, own), (near_w, beside), (far_w, across), (fwd_w, relayed)):
                    for m in range(nloc):
                        if weights[j][m] is not None:
                            acc = acc - weights[j][m] * values[m]
                total_of[j, v] = acc
        for n in range(nloc):
            b = [total_of[n, v] for v in range(NV)]
            for v in range(NV):
                res_ref[n, v, x] = b[v]
            for p in range(NV):
                for t in range(p + 1, NV):
                    b[t] = b[t] - lu[n, t, p, x] * b[p]
            for p in reversed(range(NV)):
                for j in range(p + 1, NV):
                    b[p] = b[p] - lu[n, p, j, x] * b[j]
                b[p] = b[p] * lu[n, p, p, x]
            for v in range(NV):
                plane = cur[k, x + 1, n, v] + b[v]
                out_ref[n, v, x] = plane
                cur[k + 1, x + 1, n, v] = plane
                put_rows(k + 1, x, n, v, plane)

        @pl.when(k < ITERS - 1)
        def _():
            send_plane(k + 1, x)
            send_rows(k + 1, x)

    forward_outer(0)
    forward(0)

    def one_step(step, c):
        for k in range(1, ITERS):

            @pl.when(step == (k - 1) * nx + outer_at(k - 1) + RELAY_LAG)
            def _():
                forward_outer(k)

        @pl.when(step + 1 < ITERS * nx)
        def _():
            forward(step + 1)

        compute(step)
        return c

    lax.fori_loop(0, ITERS * nx, one_step, 0)

    remote(near, near, send_sem.at[0], near_sem.at[0, 0], other_core).wait_send()
    remote(far, far, send_sem.at[1], far_sem.at[0, 0], other_chip).wait_send()
    remote(fwd, fwd, send_sem.at[2], fwd_sem.at[0, 0], other_core).wait_send()
    for d in range(2):
        sent = yrecv.at[:, :, d]
        remote(sent, sent, send_sem.at[3 + d], y_sem.at[0, 0, d], gy_high).wait_send()

    planes = near.at[0, pl.ds(0, ITERS)]
    remote(planes, planes, send_sem.at[5], gx_sem.at[0, 0], mate).wait_send()

    @pl.when(has_outer)
    def _():
        remote(planes, planes, send_sem.at[6], gx_sem.at[0, 1], outside).wait_send()


def shards(state, source, jacobian, couplings, omega):
    nloc, nv, nx, ny, nz = state.shape
    whole = pl.BlockSpec(memory_space=pltpu.HBM)
    in_hbm = functools.partial(pltpu.with_memory_space_constraint, memory_space=pltpu.HBM)
    scalars = pl.BlockSpec(memory_space=pltpu.SMEM)
    f32 = jnp.float32
    dma = pltpu.SemaphoreType.DMA
    plane = (nloc, nv, ny, nz)
    out = pltpu.VMEM(state.shape, f32)
    results = pl.pallas_call(
        kernel,
        out_shape=(out, out),
        in_specs=[whole, whole, whole, whole, scalars],
        out_specs=(pl.BlockSpec(memory_space=pltpu.VMEM),) * 2,
        scratch_shapes=[
            pltpu.VMEM((ITERS + 1, nx + 2) + plane, f32),
            pltpu.VMEM(source.shape, f32),
            pltpu.VMEM(jacobian.shape, f32),
            pltpu.VMEM(jacobian.shape, f32),
            pltpu.VMEM((ITERS, nx) + plane, f32),
            pltpu.VMEM((ITERS, nx) + plane, f32),
            pltpu.VMEM((ITERS, nx) + plane, f32),
            pltpu.VMEM((ITERS + 1, nx, 2, nloc, 8, nz), f32),
            pltpu.VMEM((ITERS, nx, 2, nloc, 8, nz), f32),
            pltpu.VMEM((6 * NV * NV, ny, nz), f32),
            pltpu.SMEM((NV, 6, NV), f32),
            dma((nx,)),
            dma,
            dma((nloc,)),
            dma((ITERS, nx)),
            dma((ITERS, nx)),
            dma((ITERS, nx)),
            dma((ITERS, nx, 2)),
            dma((ITERS, 2)),
            dma((7,)),
            dma,
            pltpu.SemaphoreType.REGULAR,
        ],
        compiler_params=pltpu.CompilerParams(collective_id=0, has_side_effects=True, vmem_limit_bytes=24 * 2**20),
    )(in_hbm(state), in_hbm(source), in_hbm(jacobian), in_hbm(jnp.transpose(couplings, (1, 0, 2))), omega)
    in_vmem = pl.BlockSpec(memory_space=pltpu.VMEM)
    return pl.pallas_call(
        write_out,
        out_shape=(jax.ShapeDtypeStruct(state.shape, f32),) * 2,
        in_specs=[in_vmem, in_vmem],
        out_specs=(pl.BlockSpec(memory_space=pl.ANY),) * 2,
        scratch_shapes=[dma((2,))],
    )(*(pltpu.with_memory_space_constraint(r, pltpu.VMEM) for r in results))


def write_out(next_ref, resid_ref, out_ref, res_ref, sems):
    copies = [
        pltpu.make_async_copy(next_ref, out_ref, sems.at[0]),
        pltpu.make_async_copy(resid_ref, res_ref, sems.at[1]),
    ]
    for copy in copies:
        copy.start()
    for copy in copies:
        copy.wait()


def solution(mesh):
    return jax.shard_map(
        shards,
        mesh=mesh,
        in_specs=(
            P("inst", None, "gx", "gy", None),
            P("inst", None, "gx", "gy", None),
            P("inst", None, None, "gx", "gy", None),
            P(),
            P(),
        ),
        out_specs=(P("inst", None, "gx", "gy", None), P("inst", None, "gx", "gy", None)),
        check_vma=False,
    )
```

```python
import functools
import math

import jax
import jax.numpy as jnp
from jax import lax
from jax.experimental import pallas as pl
from jax.experimental.pallas import tpu as pltpu
from jax.sharding import PartitionSpec as P

ITERS = 3
EARLY = 4
OUTER_FIRST, OUTER_STEP, RELAY_LAG = 3, 2, 5
NV = 5
MESH = pl.DeviceIdType.MESH


def table_value(offset, total):
    angle = math.pi * offset / total
    return 0.5 * (-1.0) ** offset * math.cos(angle) / math.sin(angle)


def kernel(
    state_ref, source_ref, jac_ref, coup_ref, omega_ref,
    out_ref, res_ref,
    cur, src, jac, lu, near, far, fwd, ysend, yrecv, cs, coup,
    load_sem, src_sem, jac_sem, near_sem, far_sem, fwd_sem, y_sem, gx_sem, send_sem, coup_sem, group_sem,
):
    inst, gx, gy = lax.axis_index("inst"), lax.axis_index("gx"), lax.axis_index("gy")
    ngx, ngy, ranks = lax.axis_size("gx"), lax.axis_size("gy"), lax.axis_size("inst")
    nloc, nx = state_ref.shape[0], state_ref.shape[2]
    total = ranks * nloc
    parity = lax.rem(inst, 2)
    other_core = (inst + 1 - 2 * parity, gx, gy)
    other_chip = (lax.rem(inst + 2, ranks), gx, gy)
    odd = lax.rem(gx, 2)
    mate = (inst, gx + 1 - 2 * odd, gy)
    outer = odd * (nx - 1)
    inner = nx - 1 - outer
    step_out = 2 * odd - 1
    has_outer = jnp.where(odd == 0, gx > 0, gx < ngx - 1)
    outside = (lax.rem(inst + 2, ranks), gx + step_out, gy)
    gy_low = (inst, gx, lax.rem(gy + ngy - 1, ngy))
    gy_high = (inst, gx, lax.rem(gy + 1, ngy))

    def outer_at(k):
        return jnp.minimum(OUTER_FIRST + OUTER_STEP * k, nx - 1)

    def plane_at(position, at):
        distance = jnp.where(position < at, nx - 1 - position, jnp.where(position > at, nx - position, 0))
        return outer + (1 - 2 * odd) * distance

    def load_state(x):
        return pltpu.make_async_copy(state_ref.at[:, :, x], cur.at[0, x + 1], load_sem.at[x])

    def remote(source, target, send, recv, device):
        return pltpu.make_async_remote_copy(
            src_ref=source, dst_ref=target, send_sem=send, recv_sem=recv,
            device_id=device, device_id_type=MESH,
        )

    def near_copy(k, x):
        return remote(cur.at[k, x + 1], near.at[k, x], send_sem.at[0], near_sem.at[k, x], other_core)

    def far_copy(k, x):
        return remote(cur.at[k, x + 1], far.at[k, x], send_sem.at[1], far_sem.at[k, x], other_chip)

    def fwd_copy(k, x):
        return remote(far.at[k, x], fwd.at[k, x], send_sem.at[2], fwd_sem.at[k, x], other_core)

    def y_copy(k, x, d):
        return remote(
            ysend.at[k, x, d], yrecv.at[k, x, d], send_sem.at[3 + d], y_sem.at[k, x, d],
            gy_high if d == 0 else gy_low,
        )

    def inner_copy(k):
        return remote(cur.at[k, inner + 1], cur.at[k, odd * (nx + 1)], send_sem.at[5], gx_sem.at[k, 0], mate)

    def outer_copy(k):
        return remote(far.at[k, outer], cur.at[k, (1 - odd) * (nx + 1)], send_sem.at[6], gx_sem.at[k, 1], outside)

    def send_plane(k, x):
        @pl.when(x == inner)
        def _():
            inner_copy(k).start()

        far_copy(k, x).start()
        near_copy(k, x).start()

    def send_rows(k, x):
        y_copy(k, x, 0).start()
        y_copy(k, x, 1).start()

    pltpu.make_async_copy(coup_ref, coup, coup_sem).start()
    def start_load(p, c):
        load_state(plane_at(p, 0)).start()
        return c

    lax.fori_loop(0, nx, start_load, 0)
    for n in range(nloc):
        pltpu.make_async_copy(jac_ref.at[n], jac.at[n], jac_sem.at[n]).start()
    pltpu.make_async_copy(source_ref, src, src_sem).start()

    even_here, odd_here = (inst - parity, gx, gy), (inst - parity + 1, gx, gy)
    even_far = (lax.rem(inst - parity + 2, ranks), gx, gy)

    def odd_core(device):
        return (device[0] - parity + 1, device[1], device[2])

    barrier = pltpu.get_barrier_semaphore()

    def greet(device):
        pl.semaphore_signal(barrier, inc=1, device_id=device, device_id_type=MESH)

    greet(even_far)

    @pl.when(parity == 1)
    def _():
        greet(even_here)

    for device in (mate, gy_low, gy_high):
        greet(odd_core(device))

    @pl.when(has_outer)
    def _():
        greet(odd_core(outside))

    @pl.when(parity == 0)
    def _():
        pl.semaphore_wait(barrier, 3)
        pl.semaphore_signal(group_sem, inc=1, device_id=odd_here, device_id_type=MESH)

    @pl.when(parity == 1)
    def _():
        pl.semaphore_wait(group_sem, 1)

    def meet_neighbours():
        @pl.when(parity == 1)
        def _():
            pl.semaphore_wait(barrier, 6 + 2 * has_outer.astype(jnp.int32))
            pl.semaphore_signal(group_sem, inc=1, device_id=even_here, device_id_type=MESH)

        @pl.when(parity == 0)
        def _():
            pl.semaphore_wait(group_sem, 1)

    def put_rows(k, x, n, v, plane):
        ysend[k, x, 0, n, v : v + 1, :] = plane[7:8, :]
        ysend[k, x, 1, n, v : v + 1, :] = plane[0:1, :]

    def first_send(p, c):
        x = plane_at(p, 0)
        load_state(x).wait()
        far_copy(0, x).start()
        near_copy(0, x).start()
        return c

    def first_rows(p, c):
        x = plane_at(p, 0)
        for n in range(nloc):
            for v in range(NV):
                put_rows(0, x, n, v, cur[0, x + 1, n, v])
        send_rows(0, x)
        return c

    lax.fori_loop(0, EARLY, first_send, 0)

    tile = cs.shape[1:]
    pltpu.make_async_copy(coup_ref, coup, coup_sem).wait()
    for d in range(6):
        for v in range(NV):
            for w in range(NV):
                cs[(d * NV + v) * NV + w] = jnp.full(tile, coup[v, d, w], jnp.float32)
    zeros = jnp.zeros(cur.shape[2:], jnp.float32)

    @pl.when(gx == 0)
    def _():
        for k in range(ITERS):
            cur[k, 0] = zeros

    @pl.when(gx == ngx - 1)
    def _():
        for k in range(ITERS):
            cur[k, nx + 1] = zeros

    for n in range(nloc):
        pltpu.make_async_copy(jac_ref.at[n], jac.at[n], jac_sem.at[n]).wait()

    def factor(x, c):
        for n in range(nloc):
            m = [[jac[n, i, j, x] for j in range(NV)] for i in range(NV)]
            for p in range(NV):
                m[p][p] = 1.0 / m[p][p]
                for t in range(p + 1, NV):
                    m[t][p] = m[t][p] * m[p][p]
                    for j in range(p + 1, NV):
                        m[t][j] = m[t][j] - m[t][p] * m[p][j]
            for i in range(NV):
                for j in range(NV):
                    lu[n, i, j, x] = m[i][j]
        return c

    lax.fori_loop(0, nx, factor, 0)
    pltpu.make_async_copy(source_ref, src, src_sem).wait()
    meet_neighbours()
    inner_copy(0).start()
    lax.fori_loop(EARLY, nx, first_send, 0)
    lax.fori_loop(0, nx, first_rows, 0)

    omega = omega_ref[0]

    def weight(even, odd):
        return omega * jnp.where(parity == 0, jnp.float32(even), jnp.float32(odd))

    value = functools.partial(table_value, total=total)
    own_w = [[None if j == m else omega * jnp.float32(value(j - m)) for m in range(nloc)] for j in range(nloc)]
    near_w = [[weight(value(j - m - 2), value(j - m + 2)) for m in range(nloc)] for j in range(nloc)]
    far_w = [[omega * jnp.float32(value(j - m + 4)) for m in range(nloc)] for j in range(nloc)]
    fwd_w = [[weight(value(j - m + 2), value(j - m - 2)) for m in range(nloc)] for j in range(nloc)]

    def forward(step):
        k = step // nx
        x = plane_at(step - k * nx, outer_at(k))

        @pl.when(x != outer)
        def _():
            far_copy(k, x).wait_recv()
            fwd_copy(k, x).start()

    def forward_outer(k):
        far_copy(k, outer).wait_recv()

        @pl.when(has_outer)
        def _():
            outer_copy(k).start()

        fwd_copy(k, outer).start()

    def compute(step):
        k = step // nx
        x = plane_at(step - k * nx, outer_at(k))
        near_copy(k, x).wait_recv()
        y_copy(k, x, 0).wait_recv()
        y_copy(k, x, 1).wait_recv()

        @pl.when(x == inner)
        def _():
            inner_copy(k).wait_recv()

        @pl.when((x == outer) & has_outer)
        def _():
            outer_copy(k).wait_recv()

        lane = lax.broadcasted_iota(jnp.int32, tile, 1)
        row = lax.broadcasted_iota(jnp.int32, tile, 0)
        ny, nz = tile
        pairs = [(n, v) for n in range(nloc) for v in range(NV)]

        def shifted(d, n, w):
            if d < 2:
                return cur[k, x + 2 * d, n, w]
            plane = cur[k, x + 1, n, w]
            if d == 2:
                return jnp.where(row == 0, yrecv[k, x, 0, n, w : w + 1, :], pltpu.roll(plane, 1, 0))
            if d == 3:
                return jnp.where(row == ny - 1, yrecv[k, x, 1, n, w : w + 1, :], pltpu.roll(plane, ny - 1, 0))
            if d == 4:
                return jnp.where(lane == 0, 0.0, pltpu.roll(plane, 1, 1))
            return jnp.where(lane == nz - 1, 0.0, pltpu.roll(plane, nz - 1, 1))

        total_of = {}
        for n, v in pairs:
            total_of[n, v] = src[n, v, x]
        for n in range(nloc):
            mine = [cur[k, x + 1, n, w] for w in range(NV)]
            for v in range(NV):
                for w in range(NV):
                    total_of[n, v] = total_of[n, v] - jac[n, v, w, x] * mine[w]
        for d in range(6):
            field = {(n, w): shifted(d, n, w) for n, w in pairs}
            for v in range(NV):
                for w in range(NV):
                    c = cs[(d * NV + v) * NV + w]
                    for n in range(nloc):
                        total_of[n, v] = total_of[n, v] - c * field[n, w]
        fwd_copy(k, x).wait_recv()
        for v in range(NV):
            own = [cur[k, x + 1, m, v] for m in range(nloc)]
            beside = [near[k, x, m, v] for m in range(nloc)]
            across = [far[k, x, m, v] for m in range(nloc)]
            relayed = [fwd[k, x, m, v] for m in range(nloc)]
            for j in range(nloc):
                acc = total_of[j, v]
                for weights, values in ((own_w, own), (near_w, beside), (far_w, across), (fwd_w, relayed)):
                    for m in range(nloc):
                        if weights[j][m] is not None:
                            acc = acc - weights[j][m] * values[m]
                total_of[j, v] = acc
        for n in range(nloc):
            b = [total_of[n, v] for v in range(NV)]
            for v in range(NV):
                res_ref[n, v, x] = b[v]
            for p in range(NV):
                for t in range(p + 1, NV):
                    b[t] = b[t] - lu[n, t, p, x] * b[p]
            for p in reversed(range(NV)):
                for j in range(p + 1, NV):
                    b[p] = b[p] - lu[n, p, j, x] * b[j]
                b[p] = b[p] * lu[n, p, p, x]
            for v in range(NV):
                plane = cur[k, x + 1, n, v] + b[v]
                out_ref[n, v, x] = plane
                cur[k + 1, x + 1, n, v] = plane
                put_rows(k + 1, x, n, v, plane)

        @pl.when(k < ITERS - 1)
        def _():
            send_plane(k + 1, x)
            send_rows(k + 1, x)

    forward_outer(0)
    forward(0)

    def one_step(step, c):
        for k in range(1, ITERS):

            @pl.when(step == (k - 1) * nx + outer_at(k - 1) + RELAY_LAG)
            def _():
                forward_outer(k)

        @pl.when(step + 1 < ITERS * nx)
        def _():
            forward(step + 1)

        compute(step)
        return c

    lax.fori_loop(0, ITERS * nx, one_step, 0)

    remote(near, near, send_sem.at[0], near_sem.at[0, 0], other_core).wait_send()
    remote(far, far, send_sem.at[1], far_sem.at[0, 0], other_chip).wait_send()
    remote(fwd, fwd, send_sem.at[2], fwd_sem.at[0, 0], other_core).wait_send()
    for d in range(2):
        sent = yrecv.at[:, :, d]
        remote(sent, sent, send_sem.at[3 + d], y_sem.at[0, 0, d], gy_high).wait_send()

    planes = near.at[0, pl.ds(0, ITERS)]
    remote(planes, planes, send_sem.at[5], gx_sem.at[0, 0], mate).wait_send()

    @pl.when(has_outer)
    def _():
        remote(planes, planes, send_sem.at[6], gx_sem.at[0, 1], outside).wait_send()


def shards(state, source, jacobian, couplings, omega):
    nloc, nv, nx, ny, nz = state.shape
    whole = pl.BlockSpec(memory_space=pltpu.HBM)
    in_hbm = functools.partial(pltpu.with_memory_space_constraint, memory_space=pltpu.HBM)
    scalars = pl.BlockSpec(memory_space=pltpu.SMEM)
    f32 = jnp.float32
    dma = pltpu.SemaphoreType.DMA
    plane = (nloc, nv, ny, nz)
    out = pltpu.VMEM(state.shape, f32)
    results = pl.pallas_call(
        kernel,
        out_shape=(out, out),
        in_specs=[whole, whole, whole, whole, scalars],
        out_specs=(pl.BlockSpec(memory_space=pltpu.VMEM),) * 2,
        scratch_shapes=[
            pltpu.VMEM((ITERS + 1, nx + 2) + plane, f32),
            pltpu.VMEM(source.shape, f32),
            pltpu.VMEM(jacobian.shape, f32),
            pltpu.VMEM(jacobian.shape, f32),
            pltpu.VMEM((ITERS, nx) + plane, f32),
            pltpu.VMEM((ITERS, nx) + plane, f32),
            pltpu.VMEM((ITERS, nx) + plane, f32),
            pltpu.VMEM((ITERS + 1, nx, 2, nloc, 8, nz), f32),
            pltpu.VMEM((ITERS, nx, 2, nloc, 8, nz), f32),
            pltpu.VMEM((6 * NV * NV, ny, nz), f32),
            pltpu.SMEM((NV, 6, NV), f32),
            dma((nx,)),
            dma,
            dma((nloc,)),
            dma((ITERS, nx)),
            dma((ITERS, nx)),
            dma((ITERS, nx)),
            dma((ITERS, nx, 2)),
            dma((ITERS, 2)),
            dma((7,)),
            dma,
            pltpu.SemaphoreType.REGULAR,
        ],
        compiler_params=pltpu.CompilerParams(collective_id=0, has_side_effects=True, vmem_limit_bytes=24 * 2**20),
    )(in_hbm(state), in_hbm(source), in_hbm(jacobian), in_hbm(jnp.transpose(couplings, (1, 0, 2))), omega)
    in_vmem = pl.BlockSpec(memory_space=pltpu.VMEM)
    return pl.pallas_call(
        write_out,
        out_shape=(jax.ShapeDtypeStruct(state.shape, f32),) * 2,
        in_specs=[in_vmem, in_vmem],
        out_specs=(pl.BlockSpec(memory_space=pl.ANY),) * 2,
        scratch_shapes=[dma((2,))],
    )(*(pltpu.with_memory_space_constraint(r, pltpu.VMEM) for r in results))


def write_out(next_ref, resid_ref, out_ref, res_ref, sems):
    copies = [
        pltpu.make_async_copy(next_ref, out_ref, sems.at[0]),
        pltpu.make_async_copy(resid_ref, res_ref, sems.at[1]),
    ]
    for copy in copies:
        copy.start()
    for copy in copies:
        copy.wait()


def solution(mesh):
    return jax.shard_map(
        shards,
        mesh=mesh,
        in_specs=(
            P("inst", None, "gx", "gy", None),
            P("inst", None, "gx", "gy", None),
            P("inst", None, None, "gx", "gy", None),
            P(),
            P(),
        ),
        out_specs=(P("inst", None, "gx", "gy", None), P("inst", None, "gx", "gy", None)),
        check_vma=False,
    )
```

```python
import functools
import math

import jax
import jax.numpy as jnp
from jax import lax
from jax.experimental import pallas as pl
from jax.experimental.pallas import tpu as pltpu
from jax.sharding import PartitionSpec as P

ITERS = 3
EARLY = 4
OUTER_FIRST, OUTER_STEP, RELAY_LAG = 3, 2, 5
NV = 5
MESH = pl.DeviceIdType.MESH


def table_value(offset, total):
    angle = math.pi * offset / total
    return 0.5 * (-1.0) ** offset * math.cos(angle) / math.sin(angle)


def kernel(
    state_ref, source_ref, jac_ref, coup_ref, omega_ref,
    out_ref, res_ref,
    cur, src, jac, lu, near, far, fwd, ysend, yrecv, cs, coup,
    load_sem, src_sem, jac_sem, near_sem, far_sem, fwd_sem, y_sem, gx_sem, send_sem, coup_sem, group_sem,
):
    inst, gx, gy = lax.axis_index("inst"), lax.axis_index("gx"), lax.axis_index("gy")
    ngx, ngy, ranks = lax.axis_size("gx"), lax.axis_size("gy"), lax.axis_size("inst")
    nloc, nx = state_ref.shape[0], state_ref.shape[2]
    total = ranks * nloc
    parity = lax.rem(inst, 2)
    other_core = (inst + 1 - 2 * parity, gx, gy)
    other_chip = (lax.rem(inst + 2, ranks), gx, gy)
    odd = lax.rem(gx, 2)
    mate = (inst, gx + 1 - 2 * odd, gy)
    outer = odd * (nx - 1)
    inner = nx - 1 - outer
    step_out = 2 * odd - 1
    has_outer = jnp.where(odd == 0, gx > 0, gx < ngx - 1)
    outside = (lax.rem(inst + 2, ranks), gx + step_out, gy)
    gy_low = (inst, gx, lax.rem(gy + ngy - 1, ngy))
    gy_high = (inst, gx, lax.rem(gy + 1, ngy))

    def outer_at(k):
        return jnp.minimum(OUTER_FIRST + OUTER_STEP * k, nx - 1)

    def plane_at(position, at):
        distance = jnp.where(position < at, nx - 1 - position, jnp.where(position > at, nx - position, 0))
        return outer + (1 - 2 * odd) * distance

    def load_state(x):
        return pltpu.make_async_copy(state_ref.at[:, :, x], cur.at[0, x + 1], load_sem.at[x])

    def remote(source, target, send, recv, device):
        return pltpu.make_async_remote_copy(
            src_ref=source, dst_ref=target, send_sem=send, recv_sem=recv,
            device_id=device, device_id_type=MESH,
        )

    def near_copy(k, x):
        return remote(cur.at[k, x + 1], near.at[k, x], send_sem.at[0], near_sem.at[k, x], other_core)

    def far_copy(k, x):
        return remote(cur.at[k, x + 1], far.at[k, x], send_sem.at[1], far_sem.at[k, x], other_chip)

    def fwd_copy(k, x):
        return remote(far.at[k, x], fwd.at[k, x], send_sem.at[2], fwd_sem.at[k, x], other_core)

    def y_copy(k, x, d):
        return remote(
            ysend.at[k, x, d], yrecv.at[k, x, d], send_sem.at[3 + d], y_sem.at[k, x, d],
            gy_high if d == 0 else gy_low,
        )

    def inner_copy(k):
        return remote(cur.at[k, inner + 1], cur.at[k, odd * (nx + 1)], send_sem.at[5], gx_sem.at[k, 0], mate)

    def outer_copy(k):
        return remote(far.at[k, outer], cur.at[k, (1 - odd) * (nx + 1)], send_sem.at[6], gx_sem.at[k, 1], outside)

    def send_plane(k, x):
        @pl.when(x == inner)
        def _():
            inner_copy(k).start()

        far_copy(k, x).start()
        near_copy(k, x).start()

    def send_rows(k, x):
        y_copy(k, x, 0).start()
        y_copy(k, x, 1).start()

    pltpu.make_async_copy(coup_ref, coup, coup_sem).start()
    def start_load(p, c):
        load_state(plane_at(p, 0)).start()
        return c

    lax.fori_loop(0, nx, start_load, 0)
    for n in range(nloc):
        pltpu.make_async_copy(jac_ref.at[n], jac.at[n], jac_sem.at[n]).start()
    pltpu.make_async_copy(source_ref, src, src_sem).start()

    even_here, odd_here = (inst - parity, gx, gy), (inst - parity + 1, gx, gy)
    even_far = (lax.rem(inst - parity + 2, ranks), gx, gy)

    def odd_core(device):
        return (device[0] - parity + 1, device[1], device[2])

    barrier = pltpu.get_barrier_semaphore()

    def greet(device):
        pl.semaphore_signal(barrier, inc=1, device_id=device, device_id_type=MESH)

    greet(even_far)

    @pl.when(parity == 1)
    def _():
        greet(even_here)

    for device in (mate, gy_low, gy_high):
        greet(odd_core(device))

    @pl.when(has_outer)
    def _():
        greet(odd_core(outside))

    @pl.when(parity == 0)
    def _():
        pl.semaphore_wait(barrier, 3)
        pl.semaphore_signal(group_sem, inc=1, device_id=odd_here, device_id_type=MESH)

    @pl.when(parity == 1)
    def _():
        pl.semaphore_wait(group_sem, 1)

    def meet_neighbours():
        @pl.when(parity == 1)
        def _():
            pl.semaphore_wait(barrier, 6 + 2 * has_outer.astype(jnp.int32))
            pl.semaphore_signal(group_sem, inc=1, device_id=even_here, device_id_type=MESH)

        @pl.when(parity == 0)
        def _():
            pl.semaphore_wait(group_sem, 1)

    def put_rows(k, x, n, v, plane):
        ysend[k, x, 0, n, v : v + 1, :] = plane[7:8, :]
        ysend[k, x, 1, n, v : v + 1, :] = plane[0:1, :]

    def first_send(p, c):
        x = plane_at(p, 0)
        load_state(x).wait()
        far_copy(0, x).start()
        near_copy(0, x).start()
        return c

    def first_rows(p, c):
        x = plane_at(p, 0)
        for n in range(nloc):
            for v in range(NV):
                put_rows(0, x, n, v, cur[0, x + 1, n, v])
        send_rows(0, x)
        return c

    lax.fori_loop(0, EARLY, first_send, 0)

    tile = cs.shape[1:]
    pltpu.make_async_copy(coup_ref, coup, coup_sem).wait()
    for d in range(6):
        for v in range(NV):
            for w in range(NV):
                cs[(d * NV + v) * NV + w] = jnp.full(tile, coup[v, d, w], jnp.float32)
    zeros = jnp.zeros(cur.shape[2:], jnp.float32)

    @pl.when(gx == 0)
    def _():
        for k in range(ITERS):
            cur[k, 0] = zeros

    @pl.when(gx == ngx - 1)
    def _():
        for k in range(ITERS):
            cur[k, nx + 1] = zeros

    for n in range(nloc):
        pltpu.make_async_copy(jac_ref.at[n], jac.at[n], jac_sem.at[n]).wait()

    def factor(x, c):
        for n in range(nloc):
            m = [[jac[n, i, j, x] for j in range(NV)] for i in range(NV)]
            for p in range(NV):
                m[p][p] = 1.0 / m[p][p]
                for t in range(p + 1, NV):
                    m[t][p] = m[t][p] * m[p][p]
                    for j in range(p + 1, NV):
                        m[t][j] = m[t][j] - m[t][p] * m[p][j]
            for i in range(NV):
                for j in range(NV):
                    lu[n, i, j, x] = m[i][j]
        return c

    lax.fori_loop(0, nx, factor, 0)
    pltpu.make_async_copy(source_ref, src, src_sem).wait()
    meet_neighbours()
    inner_copy(0).start()
    lax.fori_loop(EARLY, nx, first_send, 0)
    lax.fori_loop(0, nx, first_rows, 0)

    omega = omega_ref[0]

    def weight(even, odd):
        return omega * jnp.where(parity == 0, jnp.float32(even), jnp.float32(odd))

    value = functools.partial(table_value, total=total)
    own_w = [[None if j == m else omega * jnp.float32(value(j - m)) for m in range(nloc)] for j in range(nloc)]
    near_w = [[weight(value(j - m - 2), value(j - m + 2)) for m in range(nloc)] for j in range(nloc)]
    far_w = [[omega * jnp.float32(value(j - m + 4)) for m in range(nloc)] for j in range(nloc)]
    fwd_w = [[weight(value(j - m + 2), value(j - m - 2)) for m in range(nloc)] for j in range(nloc)]

    def forward(step):
        k = step // nx
        x = plane_at(step - k * nx, outer_at(k))

        @pl.when(x != outer)
        def _():
            far_copy(k, x).wait_recv()
            fwd_copy(k, x).start()

    def forward_outer(k):
        far_copy(k, outer).wait_recv()

        @pl.when(has_outer)
        def _():
            outer_copy(k).start()

        fwd_copy(k, outer).start()

    def compute(step):
        k = step // nx
        x = plane_at(step - k * nx, outer_at(k))
        near_copy(k, x).wait_recv()
        y_copy(k, x, 0).wait_recv()
        y_copy(k, x, 1).wait_recv()

        @pl.when(x == inner)
        def _():
            inner_copy(k).wait_recv()

        @pl.when((x == outer) & has_outer)
        def _():
            outer_copy(k).wait_recv()

        lane = lax.broadcasted_iota(jnp.int32, tile, 1)
        row = lax.broadcasted_iota(jnp.int32, tile, 0)
        ny, nz = tile
        pairs = [(n, v) for n in range(nloc) for v in range(NV)]

        def shifted(d, n, w):
            if d < 2:
                return cur[k, x + 2 * d, n, w]
            plane = cur[k, x + 1, n, w]
            if d == 2:
                return jnp.where(row == 0, yrecv[k, x, 0, n, w : w + 1, :], pltpu.roll(plane, 1, 0))
            if d == 3:
                return jnp.where(row == ny - 1, yrecv[k, x, 1, n, w : w + 1, :], pltpu.roll(plane, ny - 1, 0))
            if d == 4:
                return jnp.where(lane == 0, 0.0, pltpu.roll(plane, 1, 1))
            return jnp.where(lane == nz - 1, 0.0, pltpu.roll(plane, nz - 1, 1))

        total_of = {}
        for n, v in pairs:
            total_of[n, v] = src[n, v, x]
        for n in range(nloc):
            mine = [cur[k, x + 1, n, w] for w in range(NV)]
            for v in range(NV):
                for w in range(NV):
                    total_of[n, v] = total_of[n, v] - jac[n, v, w, x] * mine[w]
        for d in range(6):
            field = {(n, w): shifted(d, n, w) for n, w in pairs}
            for v in range(NV):
                for w in range(NV):
                    c = cs[(d * NV + v) * NV + w]
                    for n in range(nloc):
                        total_of[n, v] = total_of[n, v] - c * field[n, w]
        for v in range(NV):
            own = [cur[k, x + 1, m, v] for m in range(nloc)]
            beside = [near[k, x, m, v] for m in range(nloc)]
            across = [far[k, x, m, v] for m in range(nloc)]
            for j in range(nloc):
                acc = total_of[j, v]
                for weights, values in ((own_w, own), (near_w, beside), (far_w, across)):
                    for m in range(nloc):
                        if weights[j][m] is not None:
                            acc = acc - weights[j][m] * values[m]
                total_of[j, v] = acc
        fwd_copy(k, x).wait_recv()
        for v in range(NV):
            relayed = [fwd[k, x, m, v] for m in range(nloc)]
            for j in range(nloc):
                for m in range(nloc):
                    total_of[j, v] = total_of[j, v] - fwd_w[j][m] * relayed[m]
        for n in range(nloc):
            b = [total_of[n, v] for v in range(NV)]
            for v in range(NV):
                res_ref[n, v, x] = b[v]
            for p in range(NV):
                for t in range(p + 1, NV):
                    b[t] = b[t] - lu[n, t, p, x] * b[p]
            for p in reversed(range(NV)):
                for j in range(p + 1, NV):
                    b[p] = b[p] - lu[n, p, j, x] * b[j]
                b[p] = b[p] * lu[n, p, p, x]
            for v in range(NV):
                plane = cur[k, x + 1, n, v] + b[v]
                out_ref[n, v, x] = plane
                cur[k + 1, x + 1, n, v] = plane

        @pl.when(k < ITERS - 1)
        def _():
            for n, v in pairs:
                put_rows(k + 1, x, n, v, cur[k + 1, x + 1, n, v])
            send_plane(k + 1, x)
            send_rows(k + 1, x)

    forward_outer(0)
    forward(0)

    def one_step(step, c):
        for k in range(1, ITERS):

            @pl.when(step == (k - 1) * nx + outer_at(k - 1) + RELAY_LAG)
            def _():
                forward_outer(k)

        @pl.when(step + 1 < ITERS * nx)
        def _():
            forward(step + 1)

        compute(step)
        return c

    lax.fori_loop(0, ITERS * nx, one_step, 0)

    remote(near, near, send_sem.at[0], near_sem.at[0, 0], other_core).wait_send()
    remote(far, far, send_sem.at[1], far_sem.at[0, 0], other_chip).wait_send()
    remote(fwd, fwd, send_sem.at[2], fwd_sem.at[0, 0], other_core).wait_send()
    for d in range(2):
        sent = yrecv.at[:, :, d]
        remote(sent, sent, send_sem.at[3 + d], y_sem.at[0, 0, d], gy_high).wait_send()

    planes = near.at[0, pl.ds(0, ITERS)]
    remote(planes, planes, send_sem.at[5], gx_sem.at[0, 0], mate).wait_send()

    @pl.when(has_outer)
    def _():
        remote(planes, planes, send_sem.at[6], gx_sem.at[0, 1], outside).wait_send()


def shards(state, source, jacobian, couplings, omega):
    nloc, nv, nx, ny, nz = state.shape
    whole = pl.BlockSpec(memory_space=pltpu.HBM)
    in_hbm = functools.partial(pltpu.with_memory_space_constraint, memory_space=pltpu.HBM)
    scalars = pl.BlockSpec(memory_space=pltpu.SMEM)
    f32 = jnp.float32
    dma = pltpu.SemaphoreType.DMA
    plane = (nloc, nv, ny, nz)
    out = pltpu.VMEM(state.shape, f32)
    results = pl.pallas_call(
        kernel,
        out_shape=(out, out),
        in_specs=[whole, whole, whole, whole, scalars],
        out_specs=(pl.BlockSpec(memory_space=pltpu.VMEM),) * 2,
        scratch_shapes=[
            pltpu.VMEM((ITERS + 1, nx + 2) + plane, f32),
            pltpu.VMEM(source.shape, f32),
            pltpu.VMEM(jacobian.shape, f32),
            pltpu.VMEM(jacobian.shape, f32),
            pltpu.VMEM((ITERS, nx) + plane, f32),
            pltpu.VMEM((ITERS, nx) + plane, f32),
            pltpu.VMEM((ITERS, nx) + plane, f32),
            pltpu.VMEM((ITERS + 1, nx, 2, nloc, 8, nz), f32),
            pltpu.VMEM((ITERS, nx, 2, nloc, 8, nz), f32),
            pltpu.VMEM((6 * NV * NV, ny, nz), f32),
            pltpu.SMEM((NV, 6, NV), f32),
            dma((nx,)),
            dma,
            dma((nloc,)),
            dma((ITERS, nx)),
            dma((ITERS, nx)),
            dma((ITERS, nx)),
            dma((ITERS, nx, 2)),
            dma((ITERS, 2)),
            dma((7,)),
            dma,
            pltpu.SemaphoreType.REGULAR,
        ],
        compiler_params=pltpu.CompilerParams(collective_id=0, has_side_effects=True, vmem_limit_bytes=24 * 2**20),
    )(in_hbm(state), in_hbm(source), in_hbm(jacobian), in_hbm(jnp.transpose(couplings, (1, 0, 2))), omega)
    in_vmem = pl.BlockSpec(memory_space=pltpu.VMEM)
    return pl.pallas_call(
        write_out,
        out_shape=(jax.ShapeDtypeStruct(state.shape, f32),) * 2,
        in_specs=[in_vmem, in_vmem],
        out_specs=(pl.BlockSpec(memory_space=pl.ANY),) * 2,
        scratch_shapes=[dma((2,))],
    )(*(pltpu.with_memory_space_constraint(r, pltpu.VMEM) for r in results))


def write_out(next_ref, resid_ref, out_ref, res_ref, sems):
    copies = [
        pltpu.make_async_copy(next_ref, out_ref, sems.at[0]),
        pltpu.make_async_copy(resid_ref, res_ref, sems.at[1]),
    ]
    for copy in copies:
        copy.start()
    for copy in copies:
        copy.wait()


def solution(mesh):
    return jax.shard_map(
        shards,
        mesh=mesh,
        in_specs=(
            P("inst", None, "gx", "gy", None),
            P("inst", None, "gx", "gy", None),
            P("inst", None, None, "gx", "gy", None),
            P(),
            P(),
        ),
        out_specs=(P("inst", None, "gx", "gy", None), P("inst", None, "gx", "gy", None)),
        check_vma=False,
    )
```
